256 devices in a mesh: ulysses: 32 (over z, x), blk: 8 (over y, core).
Axes of the slice: x: 4, y: 4, z: 8, core: 2. Of those that a mesh axis runs over, the one named last changes fastest.
Arguments:
- queries: bfloat16 [16384, 4096], P(('ulysses', 'blk')), may hold values from -6 to 6
- key_rows: bfloat16 [16384, 1024], P(('ulysses', 'blk')), may hold values from -6 to 6
- value_rows: bfloat16 [16384, 1024], P(('ulysses', 'blk')), may hold values from -6 to 6
Outputs:
- attended: bfloat16 [16384, 4096], P(('ulysses', 'blk'))
The draws below stay inside these ranges and needn't reach their ends.
All inputs are finite; a program needn't handle non-finite values.
Results may differ from the reference program's by a relative error of at most 0.006.
Values may be sent and summed in bfloat16 or wider, within the bound.
No kernel may reach another device: no remote copies, remote signals or barrier semaphores. Data moves between devices by JAX's collectives and lax.ppermute only.
A program may use at most 64 MiB of HBM per device.

```python
import math
import jax
import jax.numpy as jnp
from jax import lax

Q_HEADS = 32
KV_HEADS = 8
HEAD_DIM = 128
GROUP = 4
SEQ = 16384


def draw_queries(key, part):
    raw = jax.random.normal(jax.random.fold_in(key, 1), (SEQ, Q_HEADS * HEAD_DIM), jnp.float32)
    return jnp.clip(raw, -6.0, 6.0).astype(jnp.bfloat16)


def draw_key_rows(key, part):
    raw = jax.random.normal(jax.random.fold_in(key, 3), (SEQ, KV_HEADS * HEAD_DIM), jnp.float32)
    return jnp.clip(raw, -6.0, 6.0).astype(jnp.bfloat16)


def level_of(rng, shape, cuts, smallest, high):
    def one(dim, blocks):
        steps = jax.random.uniform(jax.random.fold_in(jax.random.fold_in(rng, 6), dim), (blocks,), jnp.float32, smallest / len(cuts), high / len(cuts))
        return jnp.repeat(jnp.exp(steps), shape[dim] // blocks).reshape((-1,) + (1,) * (len(shape) - dim - 1))

    loudness = one(*cuts[0])
    for cut in cuts[1:]:
        loudness = loudness * one(*cut)
    return loudness


def centred(key, extent, scale, most, shards=(), kind=jnp.bfloat16):
    entries = jax.random.normal(key, extent, jnp.float32) * scale
    if len(shards) > 0:
        entries = level_of(key, extent, shards, -0.22, 0.18) * entries
    return jnp.clip(entries, min=-most, max=most).astype(kind)


def setup_inputs(seed: int = 0) -> dict:
    splits = jax.random.split(jax.random.key(seed), 4)
    queries = draw_queries(jax.random.fold_in(splits[3], 71), 0)
    key_rows = draw_key_rows(jax.random.fold_in(splits[3], 71), 0)
    value_rows = centred(splits[2], (SEQ, KV_HEADS * HEAD_DIM), 1.0, 6.0, ((0, 256),))
    return {"queries": queries, "key_rows": key_rows, "value_rows": value_rows}


def reference(queries, key_rows, value_rows):
    seq = queries.shape[0]
    tile_rows = min(512, seq)
    tile_count = seq // tile_rows
    scale = 1.0 / math.sqrt(HEAD_DIM)
    grouped = queries.reshape(seq, KV_HEADS, GROUP, HEAD_DIM)
    keyed = key_rows.reshape(seq, KV_HEADS, HEAD_DIM)
    valued = value_rows.reshape(seq, KV_HEADS, HEAD_DIM)
    key_where = jnp.arange(seq, dtype=jnp.int32)

    def one_tile(index):
        head = (index // tile_count).astype(jnp.int32)
        first = (index % tile_count * tile_rows).astype(jnp.int32)
        zero = jnp.zeros((), jnp.int32)
        q_part = lax.dynamic_slice(grouped, (first, head, zero, zero), (tile_rows, 1, GROUP, HEAD_DIM))[:, 0]
        k_head = lax.dynamic_slice(keyed, (zero, head, zero), (seq, 1, HEAD_DIM))[:, 0]
        v_head = lax.dynamic_slice(valued, (zero, head, zero), (seq, 1, HEAD_DIM))[:, 0]
        scores = jnp.einsum('tgd,sd->gts', q_part.astype(jnp.float32), k_head.astype(jnp.float32)) * scale
        q_where = first + jnp.arange(tile_rows, dtype=jnp.int32)
        allowed = key_where[None, :] <= q_where[:, None]
        scores = jnp.where(allowed, scores, -1e+30)
        top = lax.optimization_barrier(jnp.max(scores, axis=-1, keepdims=True))
        weights = jnp.where(allowed, jnp.exp(scores - top), 0.0)
        total = lax.optimization_barrier(jnp.sum(weights, axis=-1, keepdims=True))
        rounded = weights.astype(jnp.bfloat16)
        mixed = jnp.einsum('gts,sd->gtd', rounded.astype(jnp.float32), v_head.astype(jnp.float32)) / total
        return mixed.astype(jnp.bfloat16)
    blocks = lax.map(one_tile, jnp.arange(KV_HEADS * tile_count, dtype=jnp.int32))
    blocks = blocks.reshape(KV_HEADS, tile_count, GROUP, tile_rows, HEAD_DIM).transpose(1, 3, 0, 2, 4)
    return blocks.reshape(seq, Q_HEADS * HEAD_DIM)
```

```python
import functools
import math

import jax
import jax.numpy as jnp
import numpy as np
from jax import lax
from jax.experimental import pallas as pl
from jax.experimental.pallas import tpu as pltpu
from jax.sharding import Mesh, PartitionSpec as P


KV_HEADS = 8
GROUP = 4
HEAD_DIM = 128
SPANS = 8
SIDE = 4
MASKED = -1e30
PLANE = ("x", "y", "c")
HOPS = (1, 3, 2)

UNITS = [[(s, s) for s in range(4)], [(s, s) for s in range(4, 8)]]
_used = [0] * SPANS
for _spans in ((7, 6, 5, 4), (7, 6, 5, 4), (7, 6, 5, 4), (7, 6, 5, 4), (7, 6, 5, 3), (7, 6, 3, 2), (7, 3, 2, 1)):
    UNITS.append([(s, _used[s]) for s in _spans])
    for s in _spans:
        _used[s] += 1
assert _used == list(range(SPANS))
WIDE = 4
EXTRA = 16


def turn_kernel(table_ref, place_ref, q_ref, own_ref, partner_ref, *rest, kinds, first, last):
    if first:
        acc_ref, top_ref = rest[:2]
        rest = rest[2:]
    elif last:
        acc_ref, top_ref, out_ref = rest[:3]
        rest = rest[3:]
    else:
        _, _, acc_ref, top_ref = rest[:4]
        rest = rest[4:]
    turned_ref = rest[0]
    slots = (rest[1:4], rest[4:7])
    toks = q_ref.shape[1]
    rows = GROUP * toks
    part = own_ref.shape[0] * toks
    keys = 2 * part
    to_log2 = math.log2(math.e) / math.sqrt(HEAD_DIM)
    x, y, c = (place_ref[n] for n in range(3))

    def columns(span, lo):
        return jnp.concatenate(
            [k[:, span, :, pl.ds(lo, HEAD_DIM)].reshape(part, HEAD_DIM) for k in (own_ref, partner_ref)], axis=0
        )

    if first:
        acc_ref[...] = jnp.zeros_like(acc_ref)
        top_ref[...] = jnp.full_like(top_ref, MASKED)
    for span in range(SPANS):
        turned_ref[span, pl.ds(0, HEAD_DIM)] = columns(span, HEAD_DIM).T
        turned_ref[span, pl.ds(HEAD_DIM, EXTRA)] = jnp.ones((EXTRA, keys), jnp.bfloat16)

    place = (x * SIDE + y) * 2 + c
    ahead = lax.broadcasted_iota(jnp.int32, (toks, rows), 0) - lax.broadcasted_iota(jnp.int32, (toks, rows), 1) % toks

    def hide(s):
        pieces = []
        for n in range(keys // toks):
            mine, stage = kinds[n // SIDE]
            core = c if mine else 1 - c
            step = ((0,) + HOPS)[n % SIDE]
            near = (jnp.where(core == 0, x, y) + (SIDE - step)) % SIDE
            far = (jnp.where(core == 0, y, x) + (SIDE - stage)) % SIDE
            chip = jnp.where(core == 0, near * SIDE + far, far * SIDE + near)
            start = (chip * 2 + core - place) * toks
            pieces.append(jnp.where(ahead <= -start, s[n * toks : (n + 1) * toks], MASKED))
        return jnp.concatenate(pieces, axis=0)

    def scores(unit, t, slot, diagonal):
        score, shift, gain = slot
        tile = table_ref[0, unit * WIDE + t]
        span = table_ref[1, unit * WIDE + t]
        q = jnp.concatenate([q_ref[tile, :, pl.ds(h * HEAD_DIM, HEAD_DIM)] for h in range(GROUP)], axis=0)
        s = lax.dot_general(columns(span, 0), q, (((1,), (1,)), ((), ())), preferred_element_type=jnp.float32)
        if diagonal:
            s = hide(s)
        score[t] = s
        old = top_ref[tile]
        high = jnp.max(s.reshape(keys // 8, 8, rows), axis=0)
        new = jnp.maximum(old, jnp.broadcast_to(jnp.max(high, axis=0, keepdims=True), old.shape))
        top_ref[tile] = new
        shift[t] = new * to_log2
        gain[t] = jnp.exp2((old - new) * to_log2)

    def gather(unit, t, slot):
        score, shift, gain = slot
        tile = table_ref[0, unit * WIDE + t]
        span = table_ref[1, unit * WIDE + t]
        less = shift[t, 0:1]
        w = jnp.exp2(score[t] * to_log2 - less).astype(jnp.bfloat16)
        more = jnp.dot(turned_ref[span], w, preferred_element_type=jnp.float32)
        acc_ref[tile] = acc_ref[tile] * gain[t, 0:1] + more

    count = len(UNITS)

    def both(up, down):
        for t in range(WIDE):
            if up is not None:
                scores(up[0], t, slots[up[1]], up[2])
            if down is not None:
                gather(down[0], t, slots[down[1]])

    both((0, 0, True), None)
    both((1, 1, True), (0, 0))

    def two(i, carry):
        both((2 * i + 2, 0, False), (2 * i + 1, 1))
        both((2 * i + 3, 1, False), (2 * i + 2, 0))
        return carry

    lax.fori_loop(0, (count - 3) // 2, two, 0)
    both((count - 1, 0, False), (count - 2, 1))
    both(None, (count - 1, 0))
    if last:
        for tile in range(SPANS):
            mixed = (acc_ref[tile, pl.ds(0, HEAD_DIM)] / acc_ref[tile, pl.ds(HEAD_DIM, 1)]).T.astype(jnp.bfloat16)
            for h in range(GROUP):
                out_ref[tile, :, pl.ds(h * HEAD_DIM, HEAD_DIM)] = mixed[h * toks : (h + 1) * toks]


def turn(kinds, place, q, own, partner, state, last):
    tiles, toks, _ = q.shape
    rows = GROUP * toks
    first = state is None
    vmem = pl.BlockSpec(memory_space=pltpu.VMEM)
    smem = pl.BlockSpec(memory_space=pltpu.SMEM)
    keys = SIDE * 2 * toks
    state_shape = [
        jax.ShapeDtypeStruct((tiles, HEAD_DIM + EXTRA, rows), jnp.float32),
        jax.ShapeDtypeStruct((tiles, 8, rows), jnp.float32),
    ]
    out_shape = jax.ShapeDtypeStruct(q.shape, jnp.bfloat16) if last else state_shape
    slot = [
        pltpu.VMEM((WIDE, keys, rows), jnp.float32),
        pltpu.VMEM((WIDE, 8, rows), jnp.float32),
        pltpu.VMEM((WIDE, 8, rows), jnp.float32),
    ]
    table = jnp.asarray(np.array(UNITS, np.int32).reshape(-1, 2).T)
    scores = len(UNITS) * WIDE * rows * keys
    return pl.pallas_call(
        functools.partial(turn_kernel, kinds=kinds, first=first, last=last),
        in_specs=[smem, smem] + [vmem] * (3 if first else 5),
        out_specs=vmem if last else [vmem, vmem],
        out_shape=out_shape,
        scratch_shapes=[pltpu.VMEM((SPANS, HEAD_DIM + EXTRA, keys), jnp.bfloat16)] + slot + slot,
        input_output_aliases={} if first or last else {5: 0, 6: 1},
        compiler_params=pltpu.CompilerParams(vmem_limit_bytes=40 * 2**20),
        cost_estimate=pl.CostEstimate(flops=4 * scores * HEAD_DIM, bytes_accessed=8 * 2**20, transcendentals=scores),
    )(table, place, q, own, partner, *(() if first else state))


def hop(value, steps, phase):
    pairs = []
    for x in range(SIDE):
        for y in range(SIDE):
            for c in range(2):
                to = ((x + steps) % SIDE, y) if c == phase else (x, (y + steps) % SIDE)
                pairs.append(((x * SIDE + y) * 2 + c, (to[0] * SIDE + to[1]) * 2 + c))
    return lax.ppermute(value, PLANE, pairs)


def swap(value):
    return lax.ppermute(value, "c", [(0, 1), (1, 0)])


def after(value, *others):
    return lax.optimization_barrier((value, *others))[0]


def per_device(queries, key_rows, value_rows):
    toks = queries.shape[0]
    cols = GROUP * HEAD_DIM
    kv = jnp.concatenate(
        (key_rows.reshape(toks, KV_HEADS, HEAD_DIM), value_rows.reshape(toks, KV_HEADS, HEAD_DIM)), axis=2
    ).transpose(1, 0, 2)
    kv = lax.all_to_all(kv, "z", 0, 0, tiled=True)[None]
    q = queries.reshape(toks, KV_HEADS, cols).transpose(1, 0, 2)
    q = lax.all_to_all(q, "z", 0, 0, tiled=True)
    near = []
    for k in HOPS:
        near.append(hop(kv, k, 0))
    own = [jnp.concatenate([kv] + near, axis=0)]

    def far(k, *before):
        return hop(after(own[0], *before) if before else own[0], k, 1)

    own += [far(k) for k in HOPS[:2]]
    place = jnp.stack([lax.axis_index(a) for a in PLANE]).astype(jnp.int32)

    def swapped(n, *before):
        return swap(after(own[n], *before) if before else own[n])

    def turned(n, first, second, a, b, state):
        return turn((first, second), place, q, a, b, state, n == 3)

    partner = [swapped(0)]
    state = turned(0, (True, 0), (False, 0), own[0], partner[0], None)
    own.append(far(HOPS[2], *state))
    partner += [swapped(1, *state), swapped(2, *state)]
    state = turned(1, (True, HOPS[0]), (True, HOPS[1]), own[1], own[2], state)
    state = turned(2, (False, HOPS[0]), (False, HOPS[1]), partner[1], partner[2], state)
    partner.append(swapped(3, *state))
    out = turned(3, (True, HOPS[2]), (False, HOPS[2]), own[3], partner[3], state)
    out = lax.all_to_all(out, "z", 0, 0, tiled=True)
    return out.transpose(1, 0, 2).reshape(toks, KV_HEADS * cols)


def solution(mesh):
    grid = Mesh(mesh.devices.reshape(8, 4, 4, 2), ("z", "x", "y", "c"))
    spec = P(("z", "x", "y", "c"), None)
    return jax.shard_map(per_device, mesh=grid, in_specs=(spec,) * 3, out_specs=spec, check_vma=False)
```

```python
import functools
import math

import jax
import jax.numpy as jnp
import numpy as np
from jax import lax
from jax.experimental import pallas as pl
from jax.experimental.pallas import tpu as pltpu
from jax.sharding import Mesh, PartitionSpec as P


KV_HEADS = 8
GROUP = 4
HEAD_DIM = 128
SPANS = 8
SIDE = 4
MASKED = -1e30
PLANE = ("x", "y", "c")
HOPS = (1, 3, 2)

UNITS = [[(s, s) for s in range(4)], [(s, s) for s in range(4, 8)]]
_used = [0] * SPANS
for _spans in ((7, 6, 5, 4), (7, 6, 5, 4), (7, 6, 5, 4), (7, 6, 5, 4), (7, 6, 5, 3), (7, 6, 3, 2), (7, 3, 2, 1)):
    UNITS.append([(s, _used[s]) for s in _spans])
    for s in _spans:
        _used[s] += 1
assert _used == list(range(SPANS))
WIDE = 4
EXTRA = 16


def turn_kernel(table_ref, place_ref, q_ref, *rest, kinds, first, last):
    parts, rest = rest[: len(kinds)], rest[len(kinds) :]
    if first:
        acc_ref, top_ref = rest[:2]
        rest = rest[2:]
    elif last:
        acc_ref, top_ref, out_ref = rest[:3]
        rest = rest[3:]
    else:
        _, _, acc_ref, top_ref = rest[:4]
        rest = rest[4:]
    turned_ref = rest[0]
    slots = (rest[1:4], rest[4:7])
    toks = q_ref.shape[1]
    rows = GROUP * toks
    chips = [(mine, near, far) for mine, steps in kinds for near, far in steps]
    keys = len(chips) * toks
    to_log2 = math.log2(math.e) / math.sqrt(HEAD_DIM)
    x, y, c = (place_ref[n] for n in range(3))

    def columns(span, lo):
        return jnp.concatenate(
            [k[:, span, :, pl.ds(lo, HEAD_DIM)].reshape(k.shape[0] * toks, HEAD_DIM) for k in parts], axis=0
        )

    if first:
        acc_ref[...] = jnp.zeros_like(acc_ref)
        top_ref[...] = jnp.full_like(top_ref, MASKED)
    for span in range(SPANS):
        turned_ref[span, pl.ds(0, HEAD_DIM)] = columns(span, HEAD_DIM).T
        turned_ref[span, pl.ds(HEAD_DIM, EXTRA)] = jnp.ones((EXTRA, keys), jnp.bfloat16)

    place = (x * SIDE + y) * 2 + c
    ahead = lax.broadcasted_iota(jnp.int32, (toks, rows), 0) - lax.broadcasted_iota(jnp.int32, (toks, rows), 1) % toks

    def hide(s):
        pieces = []
        for n, (mine, near, far) in enumerate(chips):
            core = c if mine else 1 - c
            near = (jnp.where(core == 0, x, y) + (SIDE - near)) % SIDE
            far = (jnp.where(core == 0, y, x) + (SIDE - far)) % SIDE
            chip = jnp.where(core == 0, near * SIDE + far, far * SIDE + near)
            start = (chip * 2 + core - place) * toks
            pieces.append(jnp.where(ahead <= -start, s[n * toks : (n + 1) * toks], MASKED))
        return jnp.concatenate(pieces, axis=0)

    def scores(unit, t, slot, diagonal):
        score, shift, gain = slot
        tile = table_ref[0, unit * WIDE + t]
        span = table_ref[1, unit * WIDE + t]
        q = jnp.concatenate([q_ref[tile, :, pl.ds(h * HEAD_DIM, HEAD_DIM)] for h in range(GROUP)], axis=0)
        s = lax.dot_general(columns(span, 0), q, (((1,), (1,)), ((), ())), preferred_element_type=jnp.float32)
        if diagonal:
            s = hide(s)
        score[t] = s
        old = top_ref[tile]
        high = jnp.max(s.reshape(keys // 8, 8, rows), axis=0)
        new = jnp.maximum(old, jnp.broadcast_to(jnp.max(high, axis=0, keepdims=True), old.shape))
        top_ref[tile] = new
        shift[t] = new * to_log2
        gain[t] = jnp.exp2((old - new) * to_log2)

    def gather(unit, t, slot):
        score, shift, gain = slot
        tile = table_ref[0, unit * WIDE + t]
        span = table_ref[1, unit * WIDE + t]
        less = shift[t, 0:1]
        w = jnp.exp2(score[t] * to_log2 - less).astype(jnp.bfloat16)
        more = jnp.dot(turned_ref[span], w, preferred_element_type=jnp.float32)
        acc_ref[tile] = acc_ref[tile] * gain[t, 0:1] + more

    count = len(UNITS)

    def both(up, down):
        for t in range(WIDE):
            if up is not None:
                scores(up[0], t, slots[up[1]], up[2])
            if down is not None:
                gather(down[0], t, slots[down[1]])

    both((0, 0, True), None)
    both((1, 1, True), (0, 0))

    def two(i, carry):
        both((2 * i + 2, 0, False), (2 * i + 1, 1))
        both((2 * i + 3, 1, False), (2 * i + 2, 0))
        return carry

    lax.fori_loop(0, (count - 3) // 2, two, 0)
    both((count - 1, 0, False), (count - 2, 1))
    both(None, (count - 1, 0))
    if last:
        for tile in range(SPANS):
            mixed = (acc_ref[tile, pl.ds(0, HEAD_DIM)] / acc_ref[tile, pl.ds(HEAD_DIM, 1)]).T.astype(jnp.bfloat16)
            for h in range(GROUP):
                out_ref[tile, :, pl.ds(h * HEAD_DIM, HEAD_DIM)] = mixed[h * toks : (h + 1) * toks]


def turn(kinds, place, q, parts, state, last):
    tiles, toks, _ = q.shape
    rows = GROUP * toks
    first = state is None
    vmem = pl.BlockSpec(memory_space=pltpu.VMEM)
    smem = pl.BlockSpec(memory_space=pltpu.SMEM)
    keys = sum(p.shape[0] for p in parts) * toks
    state_shape = [
        jax.ShapeDtypeStruct((tiles, HEAD_DIM + EXTRA, rows), jnp.float32),
        jax.ShapeDtypeStruct((tiles, 8, rows), jnp.float32),
    ]
    out_shape = jax.ShapeDtypeStruct(q.shape, jnp.bfloat16) if last else state_shape
    slot = [
        pltpu.VMEM((WIDE, keys, rows), jnp.float32),
        pltpu.VMEM((WIDE, 8, rows), jnp.float32),
        pltpu.VMEM((WIDE, 8, rows), jnp.float32),
    ]
    table = jnp.asarray(np.array(UNITS, np.int32).reshape(-1, 2).T)
    scores = len(UNITS) * WIDE * rows * keys
    ahead = 3 + len(parts)
    return pl.pallas_call(
        functools.partial(turn_kernel, kinds=kinds, first=first, last=last),
        in_specs=[smem, smem] + [vmem] * (1 + len(parts) + (0 if first else 2)),
        out_specs=vmem if last else [vmem, vmem],
        out_shape=out_shape,
        scratch_shapes=[pltpu.VMEM((SPANS, HEAD_DIM + EXTRA, keys), jnp.bfloat16)] + slot + slot,
        input_output_aliases={} if first or last else {ahead: 0, ahead + 1: 1},
        compiler_params=pltpu.CompilerParams(vmem_limit_bytes=12 * 2**20),
        cost_estimate=pl.CostEstimate(flops=4 * scores * HEAD_DIM, bytes_accessed=8 * 2**20, transcendentals=scores),
    )(table, place, q, *parts, *(() if first else state))


def hop(value, steps, phase):
    pairs = []
    for x in range(SIDE):
        for y in range(SIDE):
            for c in range(2):
                to = ((x + steps) % SIDE, y) if c == phase else (x, (y + steps) % SIDE)
                pairs.append(((x * SIDE + y) * 2 + c, (to[0] * SIDE + to[1]) * 2 + c))
    return lax.ppermute(value, PLANE, pairs)


def swap(value):
    return lax.ppermute(value, "c", [(0, 1), (1, 0)])


def by_head(key_rows, value_rows):
    def body(key_ref, value_ref, out_ref, sems):
        copies = []
        for g in range(KV_HEADS):
            lanes = pl.ds(g * HEAD_DIM, HEAD_DIM)
            for n, ref in enumerate((key_ref, value_ref)):
                to = out_ref.at[g, :, pl.ds(n * HEAD_DIM, HEAD_DIM)]
                copies.append(pltpu.make_async_copy(ref.at[:, lanes], to, sems.at[2 * g + n]))
        for copy in copies:
            copy.start()
        for copy in copies:
            copy.wait()

    hbm = pl.BlockSpec(memory_space=pltpu.HBM)
    shape = (KV_HEADS, key_rows.shape[0], 2 * HEAD_DIM)
    return pl.pallas_call(
        body,
        in_specs=[hbm, hbm],
        out_specs=pl.BlockSpec(memory_space=pltpu.VMEM),
        out_shape=jax.ShapeDtypeStruct(shape, key_rows.dtype),
        scratch_shapes=[pltpu.SemaphoreType.DMA((2 * KV_HEADS,))],
        compiler_params=pltpu.CompilerParams(vmem_limit_bytes=60 * 2**20),
    )(key_rows, value_rows)


def after(value, *others):
    return lax.optimization_barrier((value, *others))[0]


def per_device(queries, key_rows, value_rows):
    toks = queries.shape[0]
    cols = GROUP * HEAD_DIM
    kv = by_head(key_rows, value_rows)
    kv = lax.all_to_all(kv, "z", 0, 0, tiled=True)[None]
    q = queries.reshape(toks, KV_HEADS, cols).transpose(1, 0, 2)
    q = lax.all_to_all(q, "z", 0, 0, tiled=True)

    def moved(value, steps, phase, *before):
        return hop(after(value, *before) if before else value, steps, phase)

    def swapped(value, *before):
        return swap(after(value, *before) if before else value)

    near = {k: moved(kv, k, 0) for k in HOPS}
    low = jnp.concatenate([kv, near[1]], axis=0)
    high = jnp.concatenate([near[3], near[2]], axis=0)
    low_1 = moved(low, 1, 1)
    high_3 = moved(high, 3, 1)
    high_1 = moved(high, 1, 1)
    low_3 = moved(low, 3, 1)
    low_p, high_p = swapped(low, q), swapped(high, q)
    place = jnp.stack([lax.axis_index(a) for a in PLANE]).astype(jnp.int32)

    low_2, high_2 = moved(low_1, 1, 1), moved(high_3, 3, 1)

    def low_at(far):
        return ((0, far), (1, far))

    def high_at(far):
        return ((3, far), (2, far))

    def turned(n, parts, state):
        kinds = tuple(p[:2] for p in parts)
        return turn(kinds, place, q, [p[2] for p in parts], state, n == 3)

    state = turned(
        0, [(True, low_at(0), low), (True, high_at(0), high), (True, low_at(1), low_1), (True, high_at(3), high_3)], None
    )
    nearby = [(low_at(1), low_1), (high_at(3), high_3), (high_at(1), high_1), (low_at(3), low_3)]
    nearby_p = [(False, at, swapped(value, *state)) for at, value in nearby]
    state = turned(
        1,
        [(False, low_at(0), low_p), (False, high_at(0), high_p), (True, high_at(1), high_1), (True, low_at(3), low_3)],
        state,
    )
    low_2p, high_2p = swapped(low_2, *state), swapped(high_2, *state)
    state = turned(2, nearby_p, state)
    out = turned(
        3,
        [(True, low_at(2), low_2), (True, high_at(2), high_2), (False, low_at(2), low_2p), (False, high_at(2), high_2p)],
        state,
    )
    out = lax.all_to_all(out, "z", 0, 0, tiled=True)
    return out.transpose(1, 0, 2).reshape(toks, KV_HEADS * cols)


def solution(mesh):
    grid = Mesh(mesh.devices.reshape(8, 4, 4, 2), ("z", "x", "y", "c"))
    spec = P(("z", "x", "y", "c"), None)
    return jax.shard_map(per_device, mesh=grid, in_specs=(spec,) * 3, out_specs=spec, check_vma=False)
```

```python
import functools
import math

import jax
import jax.numpy as jnp
import numpy as np
from jax import lax
from jax.experimental import pallas as pl
from jax.experimental.pallas import tpu as pltpu
from jax.sharding import Mesh, PartitionSpec as P


KV_HEADS = 8
GROUP = 4
HEAD_DIM = 128
SPANS = 8
SIDE = 4
MASKED = -1e30
PLANE = ("x", "y", "c")
HOPS = (1, 3, 2)

UNITS = [[(s, s) for s in range(4)], [(s, s) for s in range(4, 8)]]
_used = [0] * SPANS
for _spans in ((7, 6, 5, 4), (7, 6, 5, 4), (7, 6, 5, 4), (7, 6, 5, 4), (7, 6, 5, 3), (7, 6, 3, 2), (7, 3, 2, 1)):
    UNITS.append([(s, _used[s]) for s in _spans])
    for s in _spans:
        _used[s] += 1
assert _used == list(range(SPANS))
WIDE = 4
EXTRA = 8


def turn_kernel(table_ref, place_ref, q_ref, *rest, kinds, first, last):
    parts, rest = rest[: len(kinds)], rest[len(kinds) :]
    if first:
        acc_ref, top_ref = rest[:2]
        rest = rest[2:]
    elif last:
        acc_ref, top_ref, out_ref = rest[:3]
        rest = rest[3:]
    else:
        _, _, acc_ref, top_ref = rest[:4]
        rest = rest[4:]
    turned_ref = rest[0]
    slots = (rest[1:4], rest[4:7])
    toks = q_ref.shape[1]
    rows = GROUP * toks
    chips = [(mine, near, far) for mine, steps in kinds for near, far in steps]
    keys = len(chips) * toks
    to_log2 = math.log2(math.e) / math.sqrt(HEAD_DIM)
    x, y, c = (place_ref[n] for n in range(3))

    def columns(span, lo):
        return jnp.concatenate(
            [k[:, span, :, pl.ds(lo, HEAD_DIM)].reshape(k.shape[0] * toks, HEAD_DIM) for k in parts], axis=0
        )

    if first:
        acc_ref[...] = jnp.zeros_like(acc_ref)
        top_ref[...] = jnp.full_like(top_ref, MASKED)
    for span in range(SPANS):
        turned_ref[span, pl.ds(0, HEAD_DIM)] = columns(span, HEAD_DIM).T
        turned_ref[span, pl.ds(HEAD_DIM, EXTRA)] = jnp.ones((EXTRA, keys), jnp.bfloat16)

    place = (x * SIDE + y) * 2 + c
    ahead = lax.broadcasted_iota(jnp.int32, (toks, rows), 0) - lax.broadcasted_iota(jnp.int32, (toks, rows), 1) % toks

    def hide(s):
        pieces = []
        for n, (mine, near, far) in enumerate(chips):
            core = c if mine else 1 - c
            near = (jnp.where(core == 0, x, y) + (SIDE - near)) % SIDE
            far = (jnp.where(core == 0, y, x) + (SIDE - far)) % SIDE
            chip = jnp.where(core == 0, near * SIDE + far, far * SIDE + near)
            start = (chip * 2 + core - place) * toks
            pieces.append(jnp.where(ahead <= -start, s[n * toks : (n + 1) * toks], MASKED))
        return jnp.concatenate(pieces, axis=0)

    def scores(unit, t, slot, diagonal):
        score, shift, gain = slot
        tile = table_ref[0, unit * WIDE + t]
        span = table_ref[1, unit * WIDE + t]
        q = jnp.concatenate([q_ref[tile, :, pl.ds(h * HEAD_DIM, HEAD_DIM)] for h in range(GROUP)], axis=0)
        s = lax.dot_general(columns(span, 0), q, (((1,), (1,)), ((), ())), preferred_element_type=jnp.float32)
        if diagonal:
            s = hide(s)
        score[t] = s
        old = top_ref[tile]
        high = jnp.max(s.reshape(keys // 8, 8, rows), axis=0)
        new = jnp.maximum(old, jnp.broadcast_to(jnp.max(high, axis=0, keepdims=True), old.shape))
        top_ref[tile] = new
        shift[t] = new * to_log2
        gain[t] = jnp.exp2((old - new) * to_log2)

    def gather(unit, t, slot):
        score, shift, gain = slot
        tile = table_ref[0, unit * WIDE + t]
        span = table_ref[1, unit * WIDE + t]
        less = shift[t, 0:1]
        w = jnp.exp2(score[t] * to_log2 - less).astype(jnp.bfloat16)
        more = jnp.dot(turned_ref[span], w, preferred_element_type=jnp.float32)
        acc_ref[tile] = acc_ref[tile] * gain[t, 0:1] + more

    count = len(UNITS)

    def both(up, down):
        for t in range(WIDE):
            if up is not None:
                scores(up[0], t, slots[up[1]], up[2])
            if down is not None:
                gather(down[0], t, slots[down[1]])

    both((0, 0, True), None)
    both((1, 1, True), (0, 0))

    def two(i, carry):
        both((2 * i + 2, 0, False), (2 * i + 1, 1))
        both((2 * i + 3, 1, False), (2 * i + 2, 0))
        return carry

    lax.fori_loop(0, (count - 3) // 2, two, 0)
    both((count - 1, 0, False), (count - 2, 1))
    both(None, (count - 1, 0))
    if last:
        for tile in range(SPANS):
            share = 1.0 / acc_ref[tile, pl.ds(HEAD_DIM, 1)]
            mixed = (acc_ref[tile, pl.ds(0, HEAD_DIM)] * share).T.astype(jnp.bfloat16)
            for h in range(GROUP):
                out_ref[tile, :, pl.ds(h * HEAD_DIM, HEAD_DIM)] = mixed[h * toks : (h + 1) * toks]


def turn(kinds, place, q, parts, state, last):
    tiles, toks, _ = q.shape
    rows = GROUP * toks
    first = state is None
    vmem = pl.BlockSpec(memory_space=pltpu.VMEM)
    smem = pl.BlockSpec(memory_space=pltpu.SMEM)
    keys = sum(p.shape[0] for p in parts) * toks
    state_shape = [
        jax.ShapeDtypeStruct((tiles, HEAD_DIM + EXTRA, rows), jnp.float32),
        jax.ShapeDtypeStruct((tiles, 8, rows), jnp.float32),
    ]
    out_shape = jax.ShapeDtypeStruct(q.shape, jnp.bfloat16) if last else state_shape
    slot = [
        pltpu.VMEM((WIDE, keys, rows), jnp.float32),
        pltpu.VMEM((WIDE, 8, rows), jnp.float32),
        pltpu.VMEM((WIDE, 8, rows), jnp.float32),
    ]
    table = jnp.asarray(np.array(UNITS, np.int32).reshape(-1, 2).T)
    scores = len(UNITS) * WIDE * rows * keys
    ahead = 3 + len(parts)
    return pl.pallas_call(
        functools.partial(turn_kernel, kinds=kinds, first=first, last=last),
        in_specs=[smem, smem] + [vmem] * (1 + len(parts) + (0 if first else 2)),
        out_specs=vmem if last else [vmem, vmem],
        out_shape=out_shape,
        scratch_shapes=[pltpu.VMEM((SPANS, HEAD_DIM + EXTRA, keys), jnp.bfloat16)] + slot + slot,
        input_output_aliases={} if first or last else {ahead: 0, ahead + 1: 1},
        compiler_params=pltpu.CompilerParams(vmem_limit_bytes=12 * 2**20),
        cost_estimate=pl.CostEstimate(flops=4 * scores * HEAD_DIM, bytes_accessed=8 * 2**20, transcendentals=scores),
    )(table, place, q, *parts, *(() if first else state))


def hop(value, steps, phase):
    pairs = []
    for x in range(SIDE):
        for y in range(SIDE):
            for c in range(2):
                to = ((x + steps) % SIDE, y) if c == phase else (x, (y + steps) % SIDE)
                pairs.append(((x * SIDE + y) * 2 + c, (to[0] * SIDE + to[1]) * 2 + c))
    return lax.ppermute(value, PLANE, pairs)


def swap(value):
    return lax.ppermute(value, "c", [(0, 1), (1, 0)])


def by_head(key_rows, value_rows):
    def body(key_ref, value_ref, out_ref, sems):
        copies = []
        for g in range(KV_HEADS):
            lanes = pl.ds(g * HEAD_DIM, HEAD_DIM)
            for n, ref in enumerate((key_ref, value_ref)):
                to = out_ref.at[g, :, pl.ds(n * HEAD_DIM, HEAD_DIM)]
                copies.append(pltpu.make_async_copy(ref.at[:, lanes], to, sems.at[2 * g + n]))
        for copy in copies:
            copy.start()
        for copy in copies:
            copy.wait()

    hbm = pl.BlockSpec(memory_space=pltpu.HBM)
    shape = (KV_HEADS, key_rows.shape[0], 2 * HEAD_DIM)
    return pl.pallas_call(
        body,
        in_specs=[hbm, hbm],
        out_specs=pl.BlockSpec(memory_space=pltpu.VMEM),
        out_shape=jax.ShapeDtypeStruct(shape, key_rows.dtype),
        scratch_shapes=[pltpu.SemaphoreType.DMA((2 * KV_HEADS,))],
        compiler_params=pltpu.CompilerParams(vmem_limit_bytes=60 * 2**20),
    )(key_rows, value_rows)


def after(value, *others):
    return lax.optimization_barrier((value, *others))[0]


def per_device(queries, key_rows, value_rows):
    toks = queries.shape[0]
    cols = GROUP * HEAD_DIM
    kv = by_head(key_rows, value_rows)
    kv = lax.all_to_all(kv, "z", 0, 0, tiled=True)[None]
    q = queries.reshape(toks, KV_HEADS, cols).transpose(1, 0, 2)
    q = lax.all_to_all(q, "z", 0, 0, tiled=True)

    def moved(value, steps, phase, *before):
        return hop(after(value, *before) if before else value, steps, phase)

    def swapped(value, *before):
        return swap(after(value, *before) if before else value)

    near = {k: moved(kv, k, 0) for k in HOPS}
    low = jnp.concatenate([kv, near[1]], axis=0)
    high = jnp.concatenate([near[3], near[2]], axis=0)
    low_1 = moved(low, 1, 1)
    high_3 = moved(high, 3, 1)
    high_1 = moved(high, 1, 1)
    low_3 = moved(low, 3, 1)
    low_p, high_p = swapped(low, q), swapped(high, q)
    place = jnp.stack([lax.axis_index(a) for a in PLANE]).astype(jnp.int32)

    low_2, high_2 = moved(low_1, 1, 1), moved(high_3, 3, 1)

    def low_at(far):
        return ((0, far), (1, far))

    def high_at(far):
        return ((3, far), (2, far))

    def turned(n, parts, state):
        kinds = tuple(p[:2] for p in parts)
        return turn(kinds, place, q, [p[2] for p in parts], state, n == 3)

    state = turned(
        0, [(True, low_at(0), low), (True, high_at(0), high), (True, low_at(1), low_1), (True, high_at(3), high_3)], None
    )
    nearby = [(low_at(1), low_1), (high_at(3), high_3), (high_at(1), high_1), (low_at(3), low_3)]
    nearby_p = [(False, at, swapped(value, *state)) for at, value in nearby]
    state = turned(
        1,
        [(False, low_at(0), low_p), (False, high_at(0), high_p), (True, high_at(1), high_1), (True, low_at(3), low_3)],
        state,
    )
    low_2p, high_2p = swapped(low_2, *state), swapped(high_2, *state)
    state = turned(2, nearby_p, state)
    out = turned(
        3,
        [(True, low_at(2), low_2), (True, high_at(2), high_2), (False, low_at(2), low_2p), (False, high_at(2), high_2p)],
        state,
    )
    out = lax.all_to_all(out, "z", 0, 0, tiled=True)
    return out.transpose(1, 0, 2).reshape(toks, KV_HEADS * cols)


def solution(mesh):
    grid = Mesh(mesh.devices.reshape(8, 4, 4, 2), ("z", "x", "y", "c"))
    spec = P(("z", "x", "y", "c"), None)
    return jax.shard_map(per_device, mesh=grid, in_specs=(spec,) * 3, out_specs=spec, check_vma=False)
```
